32 devices in a mesh: py: 8 (over y, x, core), pz: 4 (over z).
Axes of the slice: x: 2, y: 2, z: 4, core: 2. Of those that a mesh axis runs over, the one named last changes fastest.
Arguments:
- velocity: float32 [3, 8, 1024, 1024], P(None, 'py', 'pz'), may hold values from -14 to 14
Outputs:
- nu_t: float32 [8, 1024, 1024], P('py', 'pz')
- filtered_velocity: bfloat16 [3, 8, 1024, 1024], P(None, 'py', None, 'pz')
The draws below stay inside these ranges and needn't reach their ends.
All inputs are finite; a program needn't handle non-finite values.
Results may differ from the reference program's by a relative error of at most 0.012.
The reference program's roundings to bfloat16 on the way count: a program that leaves them out, or rounds other values in their place, can miss the bound.
Values may be sent and summed in bfloat16 or wider, within the bound.
A program may use at most 64 MiB of HBM per device.

```python
import math
import jax
import jax.numpy as jnp
import numpy as np
from jax import lax

NX = 1024
NZ = 1024
NY = 8


def draw_velocity(key, part):
    base = jax.random.fold_in(key, 17)
    noise_key, span_key, stream_key = jax.random.split(base, 3)
    heights = (jnp.arange(NY, dtype=jnp.float32) + 0.5) * (2.0 / NY) - 1.0
    profile = 1.5 * (1.0 - heights * heights)
    offset = jnp.stack([profile, jnp.zeros_like(profile), jnp.zeros_like(profile)])[:, :, None, None]
    span_frac = jnp.arange(NZ, dtype=jnp.float32) / NZ
    span_scale = jnp.exp(jnp.log(3.0) * span_frac + jax.random.uniform(span_key, (NZ,), jnp.float32, 0.0, jnp.log(1.8)))
    stream_scale = jnp.exp(jax.random.uniform(stream_key, (NX,), jnp.float32, 0.0, jnp.log(1.8)))
    amplitude = 0.25 * span_scale[:, None] * stream_scale[None, :]
    values = jnp.clip(jax.random.normal(noise_key, (3, NY, NZ, NX), jnp.float32), -5.0, 5.0) * amplitude
    return values + offset


def setup_inputs(seed: int = 0) -> dict:
    splits = jax.random.split(jax.random.key(seed), 2)
    return {
        "velocity": draw_velocity(jax.random.fold_in(splits[1], 71), 0),
    }


index_pairs = ((0, 0), (1, 1), (2, 2), (0, 1), (0, 2), (1, 2))
pair_weights = (1.0, 1.0, 1.0, 2.0, 2.0, 2.0)
epsilon = 1e-06

def filter_table(length):
    offsets = np.arange(length, dtype=np.int64)
    wavenumbers = np.arange(1, length // 4, dtype=np.int64)
    phase = offsets[:, None] * wavenumbers[None, :] % length
    kernel = (1.0 + 2.0 * np.cos(phase * (2.0 * math.pi / length)).sum(axis=1)) / length
    kernel = kernel.astype(np.float32)
    lagged = (offsets[:, None] - offsets[None, :]) % length
    return jnp.asarray(kernel[lagged], dtype=jnp.float32).astype(jnp.bfloat16)

def smooth_fields(fields, table_x, table_z):
    fields = lax.optimization_barrier(fields)
    along_x = jnp.einsum('fzx,xv->fzv', fields.astype(jnp.float32), table_x.astype(jnp.float32), precision=lax.Precision.HIGHEST).astype(jnp.bfloat16)
    along_x = lax.optimization_barrier(along_x)
    return jnp.einsum('wz,fzx->fwx', table_z.astype(jnp.float32), along_x.astype(jnp.float32), precision=lax.Precision.HIGHEST).astype(jnp.bfloat16)

def row_slopes(rows):
    rows = rows.astype(jnp.float32)
    center = rows[:, 1]
    slope_x = (jnp.roll(center, -1, 2) - jnp.roll(center, 1, 2)) * 0.5
    slope_z = (jnp.roll(center, -1, 1) - jnp.roll(center, 1, 1)) * 0.5
    slope_y = (rows[:, 2] - rows[:, 0]) * 0.5
    return (slope_x, slope_y, slope_z)

def strain(gradients):
    strain_parts = [0.5 * (gradients[b][a] + gradients[a][b]) for a, b in index_pairs]
    squares_sum = pair_weights[0] * strain_parts[0] * strain_parts[0]
    for weight, part_value in zip(pair_weights[1:], strain_parts[1:]):
        squares_sum = squares_sum + weight * part_value * part_value
    return (strain_parts, jnp.sqrt(2.0 * squares_sum))

def reference(velocity):
    table_x = filter_table(NX)
    table_z = filter_table(NZ)
    wall_rows = jnp.zeros((3, 1, NZ, NX), velocity.dtype)
    velocity_padded = jnp.concatenate([wall_rows, velocity, wall_rows], axis=1)

    def first_pass(row):
        center = lax.dynamic_slice_in_dim(velocity, row, 1, 1)[:, 0]
        return smooth_fields(center.astype(jnp.bfloat16), table_x, table_z)
    filtered_rows = lax.map(first_pass, jnp.arange(NY, dtype=jnp.int32))
    filtered_velocity = jnp.transpose(filtered_rows, (1, 0, 2, 3))
    wall_filtered = jnp.zeros((3, 1, NZ, NX), filtered_velocity.dtype)
    filtered_padded = jnp.concatenate([wall_filtered, filtered_velocity, wall_filtered], axis=1)

    def second_pass(row):
        rows_velocity = lax.dynamic_slice_in_dim(velocity_padded, row, 3, 1)
        rows_filtered = lax.dynamic_slice_in_dim(filtered_padded, row, 3, 1).astype(jnp.float32)
        strain_parts, magnitude = strain(row_slopes(rows_velocity))
        center = rows_velocity[:, 1]
        pieces = [(center[a] * center[b]).astype(jnp.bfloat16) for a, b in index_pairs]
        pieces = pieces + [(magnitude * part_value).astype(jnp.bfloat16) for part_value in strain_parts]
        smoothed = smooth_fields(jnp.stack(pieces), table_x, table_z).astype(jnp.float32)
        hat_parts, magnitude_hat = strain(row_slopes(rows_filtered))
        smooth_velocity = rows_filtered[:, 1]
        numerator = jnp.zeros_like(magnitude)
        denominator = jnp.zeros_like(magnitude)
        for pair_index, (a, b) in enumerate(index_pairs):
            leonard = smoothed[pair_index] - smooth_velocity[a] * smooth_velocity[b]
            model_term = smoothed[6 + pair_index] - 4.0 * magnitude_hat * hat_parts[pair_index]
            numerator = numerator + pair_weights[pair_index] * leonard * model_term
            denominator = denominator + pair_weights[pair_index] * model_term * model_term
        return (jnp.sum(numerator), jnp.sum(denominator), magnitude)
    numerator, denominator, magnitude = lax.map(second_pass, jnp.arange(NY, dtype=jnp.int32))
    plane_cells = NX * NZ
    coefficient = numerator / plane_cells / (2.0 * (denominator / plane_cells + epsilon))
    nu_t = coefficient[:, None, None] * magnitude
    return (nu_t, filtered_velocity)
```

```python
import functools
import math

import jax
import jax.numpy as jnp
import numpy as np
from jax import lax
from jax.experimental import pallas as pl
from jax.experimental.pallas import tpu as pltpu
from jax.sharding import PartitionSpec as P

index_pairs = ((0, 0), (1, 1), (2, 2), (0, 1), (0, 2), (1, 2))
pair_weights = (1.0, 1.0, 1.0, 2.0, 2.0, 2.0)
epsilon = 1e-06


def neighbours(first, last, axis, wrap):
    n = lax.axis_size(axis)
    up = [(i, (i + 1) % n) for i in range(n) if wrap or i + 1 < n]
    down = [(j, i) for i, j in up]
    return lax.ppermute(last, axis, up), lax.ppermute(first, axis, down)


def filter_table(length):
    offsets = np.arange(length, dtype=np.int64)
    wavenumbers = np.arange(1, length // 4, dtype=np.int64)
    phase = offsets[:, None] * wavenumbers[None, :] % length
    kernel = (1.0 + 2.0 * np.cos(phase * (2.0 * math.pi / length)).sum(axis=1)) / length
    kernel = kernel.astype(np.float32)
    lagged = (offsets[:, None] - offsets[None, :]) % length
    return jnp.asarray(kernel[lagged], dtype=jnp.float32).astype(jnp.bfloat16)


def strain(gradients):
    strain_parts = [0.5 * (gradients[b][a] + gradients[a][b]) for a, b in index_pairs]
    squares_sum = pair_weights[0] * strain_parts[0] * strain_parts[0]
    for weight, part_value in zip(pair_weights[1:], strain_parts[1:]):
        squares_sum = squares_sum + weight * part_value * part_value
    return strain_parts, jnp.sqrt(2.0 * squares_sum)


def filter_z_kernel(n, *refs):
    table, blocks, out = refs[0], refs[1 : 1 + n], refs[1 + n]
    width = blocks[0].shape[1]
    rows = min(512, out.shape[1])
    for top in range(0, out.shape[1], rows):
        total = None
        for s in range(n):
            term = jnp.dot(
                table[top : top + rows, s * width : (s + 1) * width],
                blocks[s][0],
                preferred_element_type=jnp.float32,
            )
            total = term if total is None else total + term
        out[0, top : top + rows, :] = total.astype(out.dtype)


def filter_z(table, blocks):
    n, (fields, width, columns) = len(blocks), blocks[0].shape
    length = table.shape[0]
    return pl.pallas_call(
        functools.partial(filter_z_kernel, n),
        grid=(fields,),
        in_specs=[pl.BlockSpec(table.shape, lambda f: (0, 0), pipeline_mode=pl.Buffered(1))]
        + [pl.BlockSpec((1, width, columns), lambda f: (f, 0, 0))] * n,
        out_specs=pl.BlockSpec((1, length, columns), lambda f: (f, 0, 0)),
        out_shape=jax.ShapeDtypeStruct((fields, length, columns), jnp.bfloat16),
        cost_estimate=pl.CostEstimate(
            flops=2 * fields * length * length * columns,
            bytes_accessed=4 * fields * length * columns + 2 * length * length,
            transcendentals=0,
        ),
    )(table, *blocks)


def body(velocity):
    n, me = lax.axis_size("pz"), lax.axis_index("pz")
    v = velocity[:, 0]
    depth, nx = v.shape[1:]
    nz, width = depth * n, nx // n
    table_x, table_z = filter_table(nx), filter_table(nz)
    to_x = [
        lax.dynamic_slice_in_dim(table_x, lax.rem(me + s, n) * width, width, 1) for s in range(n)
    ]
    from_z = jnp.concatenate(
        [
            lax.dynamic_slice_in_dim(table_z, lax.rem(me - s + n, n) * depth, depth, 1)
            for s in range(n)
        ],
        axis=1,
    )
    order = list(range(n - 1, 0, -1))
    order.sort(key=lambda s: -min(s, n - s))

    def exchange(pieces):
        fields = jnp.stack([p.astype(jnp.bfloat16) for p in pieces])
        blocks = [None] * n
        for s in order + [0]:
            along = jnp.einsum(
                "fzx,xv->fzv", fields, to_x[s], preferred_element_type=jnp.float32
            ).astype(jnp.bfloat16)
            if s:
                along = lax.ppermute(along, "pz", [(i, (i + s) % n) for i in range(n)])
            blocks[s] = along
        return blocks

    blocks_v = exchange([v[a] for a in range(3)])
    below, above = neighbours(v, v, "py", False)
    before, after = neighbours(v[:, :1], v[:, -1:], "pz", True)
    blocks_p = exchange([v[a] * v[b] for a, b in index_pairs])

    padded = jnp.concatenate([before, v, after], axis=1)
    slope_x = (jnp.roll(v, -1, 2) - jnp.roll(v, 1, 2)) * 0.5
    slope_y = (above - below) * 0.5
    slope_z = (padded[:, 2:] - padded[:, :-2]) * 0.5
    grad = [[slope_x[a], slope_y[a], slope_z[a]] for a in range(3)]
    parts, magnitude = strain([[g[b] for b in range(3)] for g in grad])
    blocks_s = [exchange([magnitude * p for p in parts[i : i + 3]]) for i in (0, 3)]

    hat = filter_z(from_z, blocks_v)
    below, above = neighbours(hat, hat, "py", False)
    before, after = neighbours(hat[:, :, :1], hat[:, :, -1:], "pz", True)
    u = hat.astype(jnp.float32)
    padded = jnp.concatenate([before, hat, after], axis=2).astype(jnp.float32)
    slope_x = (padded[:, :, 2:] - padded[:, :, :-2]) * 0.5
    slope_y = (above.astype(jnp.float32) - below.astype(jnp.float32)) * 0.5
    slope_z = (jnp.roll(u, -1, 1) - jnp.roll(u, 1, 1)) * 0.5
    hat_parts, magnitude_hat = strain([[slope_x[a], slope_y[a], slope_z[a]] for a in range(3)])
    products = filter_z(from_z, blocks_p)
    leonard = [
        products[p].astype(jnp.float32) - u[a] * u[b] for p, (a, b) in enumerate(index_pairs)
    ]
    coarse = [4.0 * magnitude_hat * part for part in hat_parts]

    numerator, denominator = 0.0, 0.0
    for half, blocks in enumerate(blocks_s):
        fine = filter_z(from_z, blocks).astype(jnp.float32)
        for i in range(3):
            p = 3 * half + i
            model = fine[i] - coarse[p]
            numerator = numerator + pair_weights[p] * jnp.sum(leonard[p] * model)
            denominator = denominator + pair_weights[p] * jnp.sum(model * model)
    sums = lax.psum(jnp.stack([numerator, denominator]), "pz")
    cells = nx * nz
    coefficient = sums[0] / cells / (2.0 * (sums[1] / cells + epsilon))
    return (coefficient * magnitude)[None], hat[:, None]


def solution(mesh):
    in_specs = (P(None, "py", "pz", None),)
    out_specs = (P("py", "pz", None), P(None, "py", None, "pz"))
    return jax.shard_map(body, mesh=mesh, in_specs=in_specs, out_specs=out_specs, check_vma=False)
```

```python
import functools
import math

import jax
import jax.numpy as jnp
import numpy as np
from jax import lax
from jax.experimental import pallas as pl
from jax.experimental.pallas import tpu as pltpu
from jax.sharding import PartitionSpec as P

index_pairs = ((0, 0), (1, 1), (2, 2), (0, 1), (0, 2), (1, 2))
pair_weights = (1.0, 1.0, 1.0, 2.0, 2.0, 2.0)
epsilon = 1e-06


def neighbours(first, last, axis, wrap):
    n = lax.axis_size(axis)
    up = [(i, (i + 1) % n) for i in range(n) if wrap or i + 1 < n]
    down = [(j, i) for i, j in up]
    return lax.ppermute(last, axis, up), lax.ppermute(first, axis, down)


def filter_table(length):
    offsets = np.arange(length, dtype=np.int64)
    wavenumbers = np.arange(1, length // 4, dtype=np.int64)
    phase = offsets[:, None] * wavenumbers[None, :] % length
    kernel = (1.0 + 2.0 * np.cos(phase * (2.0 * math.pi / length)).sum(axis=1)) / length
    kernel = kernel.astype(np.float32)
    lagged = (offsets[:, None] - offsets[None, :]) % length
    return jnp.asarray(kernel[lagged], dtype=jnp.float32).astype(jnp.bfloat16)


def strain(gradients):
    strain_parts = [0.5 * (gradients[b][a] + gradients[a][b]) for a, b in index_pairs]
    squares_sum = pair_weights[0] * strain_parts[0] * strain_parts[0]
    for weight, part_value in zip(pair_weights[1:], strain_parts[1:]):
        squares_sum = squares_sum + weight * part_value * part_value
    return strain_parts, jnp.sqrt(2.0 * squares_sum)


def filter_z_kernel(n, *refs):
    table, blocks, out = refs[0], refs[1 : 1 + n], refs[1 + n]
    width = blocks[0].shape[1]
    rows = min(512, out.shape[1])
    for top in range(0, out.shape[1], rows):
        total = None
        for s in range(n):
            term = jnp.dot(
                table[top : top + rows, s * width : (s + 1) * width],
                blocks[s][0],
                preferred_element_type=jnp.float32,
            )
            total = term if total is None else total + term
        out[0, top : top + rows, :] = total.astype(out.dtype)


def filter_z(table, blocks):
    n, (fields, width, columns) = len(blocks), blocks[0].shape
    length = table.shape[0]
    return pl.pallas_call(
        functools.partial(filter_z_kernel, n),
        grid=(fields,),
        in_specs=[pl.BlockSpec(table.shape, lambda f: (0, 0), pipeline_mode=pl.Buffered(1))]
        + [pl.BlockSpec((1, width, columns), lambda f: (f, 0, 0))] * n,
        out_specs=pl.BlockSpec((1, length, columns), lambda f: (f, 0, 0)),
        out_shape=jax.ShapeDtypeStruct((fields, length, columns), jnp.bfloat16),
        cost_estimate=pl.CostEstimate(
            flops=2 * fields * length * length * columns,
            bytes_accessed=4 * fields * length * columns + 2 * length * length,
            transcendentals=0,
        ),
    )(table, *blocks)


def lilly_kernel(n, weight, *refs):
    table, blocks, (leonard, coarse, start, out) = refs[0], refs[1 : 1 + n], refs[1 + n :]
    width, columns = blocks[0].shape[1:]
    rows = min(256, leonard.shape[1])

    @pl.when(pl.program_id(0) == 0)
    def _():
        out[...] = start[...]

    for top in range(0, leonard.shape[1], rows):
        total = None
        for s in range(n):
            term = jnp.dot(
                table[top : top + rows, s * width : (s + 1) * width],
                blocks[s][0],
                preferred_element_type=jnp.float32,
            )
            total = term if total is None else total + term
        fine = total.astype(jnp.bfloat16).astype(jnp.float32)
        model = fine - coarse[0, top : top + rows, :]
        for i, value in enumerate((leonard[0, top : top + rows, :] * model, model * model)):
            out[i] += weight * jnp.sum(value.reshape(rows // 8, 8, columns), axis=0)


def lilly(table, blocks, leonard, coarse, weight, start):
    n, (fields, width, columns) = len(blocks), blocks[0].shape
    length = table.shape[0]
    plane = pl.BlockSpec((1, length, columns), lambda f: (f, 0, 0))
    sums = pl.BlockSpec(start.shape, lambda f: (0, 0, 0))
    return pl.pallas_call(
        functools.partial(lilly_kernel, n, weight),
        grid=(fields,),
        in_specs=[pl.BlockSpec(table.shape, lambda f: (0, 0), pipeline_mode=pl.Buffered(1))]
        + [pl.BlockSpec((1, width, columns), lambda f: (f, 0, 0))] * n
        + [plane, plane, sums],
        out_specs=sums,
        out_shape=jax.ShapeDtypeStruct(start.shape, jnp.float32),
        cost_estimate=pl.CostEstimate(
            flops=2 * fields * length * length * columns,
            bytes_accessed=10 * fields * length * columns + 2 * length * length,
            transcendentals=0,
        ),
    )(table, *blocks, leonard, coarse, start)


def coefficient_kernel(n, cells, part, out, held, send_sem, recv_sem):
    me = lax.axis_index("pz")
    barrier = pltpu.get_barrier_semaphore()
    others = [lax.rem(me + s, n) for s in range(1, n)]
    for other in others:
        pl.semaphore_signal(
            barrier, inc=1, device_id={"pz": other}, device_id_type=pl.DeviceIdType.MESH
        )
    pl.semaphore_wait(barrier, n - 1)
    copies = [
        pltpu.make_async_remote_copy(
            src_ref=part,
            dst_ref=held.at[s],
            send_sem=send_sem.at[s],
            recv_sem=recv_sem.at[s],
            device_id={"pz": other},
            device_id_type=pl.DeviceIdType.MESH,
        )
        for s, other in enumerate(others)
    ]
    for copy in copies:
        copy.start()
    total = part[...]
    for s, copy in enumerate(copies):
        copy.wait()
        total = total + held[s]
    mean = jnp.sum(jnp.sum(total, axis=2, keepdims=True), axis=1, keepdims=True) / cells
    value = mean[0] / (2.0 * (mean[1] + epsilon))
    out[...] = jnp.broadcast_to(value, out.shape)


def coefficient_of(part, cells):
    n = lax.axis_size("pz")
    return pl.pallas_call(
        functools.partial(coefficient_kernel, n, cells),
        in_specs=[pl.BlockSpec(memory_space=pltpu.VMEM)],
        out_specs=pl.BlockSpec(memory_space=pltpu.VMEM),
        out_shape=jax.ShapeDtypeStruct((8, 128), jnp.float32),
        scratch_shapes=[
            pltpu.VMEM((n - 1,) + part.shape, jnp.float32),
            pltpu.SemaphoreType.DMA((n - 1,)),
            pltpu.SemaphoreType.DMA((n - 1,)),
        ],
        compiler_params=pltpu.CompilerParams(collective_id=0, has_side_effects=True),
    )(part)


def body(velocity):
    n, me = lax.axis_size("pz"), lax.axis_index("pz")
    v = velocity[:, 0]
    depth, nx = v.shape[1:]
    nz, width = depth * n, nx // n
    table_x, table_z = filter_table(nx), filter_table(nz)
    to_x = [
        lax.dynamic_slice_in_dim(table_x, lax.rem(me + s, n) * width, width, 1) for s in range(n)
    ]
    from_z = jnp.concatenate(
        [
            lax.dynamic_slice_in_dim(table_z, lax.rem(me - s + n, n) * depth, depth, 1)
            for s in range(n)
        ],
        axis=1,
    )
    order = list(range(n - 1, 0, -1))
    order.sort(key=lambda s: -min(s, n - s))

    def exchange(pieces):
        fields = jnp.stack([p.astype(jnp.bfloat16) for p in pieces])
        blocks = [None] * n
        for s in order + [0]:
            along = jnp.einsum(
                "fzx,xv->fzv", fields, to_x[s], preferred_element_type=jnp.float32
            ).astype(jnp.bfloat16)
            if s:
                along = lax.ppermute(along, "pz", [(i, (i + s) % n) for i in range(n)])
            blocks[s] = along
        return blocks

    blocks_v = exchange([v[a] for a in range(3)])
    below, above = neighbours(v, v, "py", False)
    before, after = neighbours(v[:, :1], v[:, -1:], "pz", True)
    blocks_p = exchange([v[a] * v[b] for a, b in index_pairs])

    padded = jnp.concatenate([before, v, after], axis=1)
    slope_x = (jnp.roll(v, -1, 2) - jnp.roll(v, 1, 2)) * 0.5
    slope_y = (above - below) * 0.5
    slope_z = (padded[:, 2:] - padded[:, :-2]) * 0.5
    grad = [[slope_x[a], slope_y[a], slope_z[a]] for a in range(3)]
    parts, magnitude = strain([[g[b] for b in range(3)] for g in grad])
    blocks_s = [exchange([magnitude * p for p in parts[i : i + 3]]) for i in (0, 3)]

    from_z, *local = lax.optimization_barrier((from_z, blocks_s[0][0], blocks_s[1][0]))
    for half in range(2):
        blocks_s[half][0] = local[half]

    hat = filter_z(from_z, blocks_v)
    below, above = neighbours(hat, hat, "py", False)
    before, after = neighbours(hat[:, :, :1], hat[:, :, -1:], "pz", True)
    u = hat.astype(jnp.float32)
    padded = jnp.concatenate([before, hat, after], axis=2).astype(jnp.float32)
    slope_x = (padded[:, :, 2:] - padded[:, :, :-2]) * 0.5
    slope_y = (above.astype(jnp.float32) - below.astype(jnp.float32)) * 0.5
    slope_z = (jnp.roll(u, -1, 1) - jnp.roll(u, 1, 1)) * 0.5
    hat_parts, magnitude_hat = strain([[slope_x[a], slope_y[a], slope_z[a]] for a in range(3)])
    products = filter_z(from_z, blocks_p)
    leonard = [
        products[p].astype(jnp.float32) - u[a] * u[b] for p, (a, b) in enumerate(index_pairs)
    ]
    coarse = [4.0 * magnitude_hat * part for part in hat_parts]

    sums = jnp.zeros((2, 8, width), jnp.float32)
    for half, blocks in enumerate(blocks_s):
        chosen = slice(3 * half, 3 * half + 3)
        sums = lilly(
            from_z,
            blocks,
            jnp.stack(leonard[chosen]),
            jnp.stack(coarse[chosen]),
            pair_weights[3 * half],
            sums,
        )
    coefficient = coefficient_of(sums, nx * nz)[0, 0]
    return (coefficient * magnitude)[None], hat[:, None]


def solution(mesh):
    in_specs = (P(None, "py", "pz", None),)
    out_specs = (P("py", "pz", None), P(None, "py", None, "pz"))
    return jax.shard_map(body, mesh=mesh, in_specs=in_specs, out_specs=out_specs, check_vma=False)
```

```python
import functools
import math

import jax
import jax.numpy as jnp
import numpy as np
from jax import lax
from jax.experimental import pallas as pl
from jax.experimental.pallas import tpu as pltpu
from jax.sharding import PartitionSpec as P

index_pairs = ((0, 0), (1, 1), (2, 2), (0, 1), (0, 2), (1, 2))
pair_weights = (1.0, 1.0, 1.0, 2.0, 2.0, 2.0)
epsilon = 1e-06


def neighbours(first, last, axis, wrap):
    n = lax.axis_size(axis)
    up = [(i, (i + 1) % n) for i in range(n) if wrap or i + 1 < n]
    down = [(j, i) for i, j in up]
    return lax.ppermute(last, axis, up), lax.ppermute(first, axis, down)


def filter_table(length):
    offsets = np.arange(length, dtype=np.int64)
    wavenumbers = np.arange(1, length // 4, dtype=np.int64)
    phase = offsets[:, None] * wavenumbers[None, :] % length
    kernel = (1.0 + 2.0 * np.cos(phase * (2.0 * math.pi / length)).sum(axis=1)) / length
    kernel = kernel.astype(np.float32)
    lagged = (offsets[:, None] - offsets[None, :]) % length
    return jnp.asarray(kernel[lagged], dtype=jnp.float32).astype(jnp.bfloat16)


def strain(gradients):
    strain_parts = [0.5 * (gradients[b][a] + gradients[a][b]) for a, b in index_pairs]
    squares_sum = pair_weights[0] * strain_parts[0] * strain_parts[0]
    for weight, part_value in zip(pair_weights[1:], strain_parts[1:]):
        squares_sum = squares_sum + weight * part_value * part_value
    return strain_parts, jnp.sqrt(2.0 * squares_sum)


def filter_z_kernel(n, *refs):
    table, blocks, out = refs[0], refs[1 : 1 + n], refs[1 + n]
    width = blocks[0].shape[1]
    rows = min(512, out.shape[1])
    for top in range(0, out.shape[1], rows):
        total = None
        for s in range(n):
            term = jnp.dot(
                table[top : top + rows, s * width : (s + 1) * width],
                blocks[s][0],
                preferred_element_type=jnp.float32,
            )
            total = term if total is None else total + term
        out[0, top : top + rows, :] = total.astype(out.dtype)


def filter_z(table, blocks):
    n, (fields, width, columns) = len(blocks), blocks[0].shape
    length = table.shape[0]
    return pl.pallas_call(
        functools.partial(filter_z_kernel, n),
        grid=(fields,),
        in_specs=[pl.BlockSpec(table.shape, lambda f: (0, 0), pipeline_mode=pl.Buffered(1))]
        + [pl.BlockSpec((1, width, columns), lambda f: (f, 0, 0))] * n,
        out_specs=pl.BlockSpec((1, length, columns), lambda f: (f, 0, 0)),
        out_shape=jax.ShapeDtypeStruct((fields, length, columns), jnp.bfloat16),
        cost_estimate=pl.CostEstimate(
            flops=2 * fields * length * length * columns,
            bytes_accessed=4 * fields * length * columns + 2 * length * length,
            transcendentals=0,
        ),
    )(table, *blocks)


def coarse_kernel(hat, below, above, before, after, out, u):
    length, columns = hat.shape[1:]
    rows = min(64, length)
    for a in range(3):
        u[a, 8 : 8 + length, :] = hat[a].astype(jnp.float32)
        u[a, 0:8, :] = hat[a, length - 16 : length, :].astype(jnp.float32)[8:]
        u[a, 8 + length : 16 + length, :] = hat[a, 0:16, :].astype(jnp.float32)[:8]
    lane = lax.broadcasted_iota(jnp.int32, (rows, columns), 1)

    def tile(i, carry):
        top = pl.multiple_of(i * rows, rows)
        here = pl.ds(top, rows)
        grad = []
        for a in range(3):
            around = u[a, pl.ds(top, rows + 16), :]
            centre = around[8 : 8 + rows]
            left, right = pltpu.roll(centre, 1, 1), pltpu.roll(centre, columns - 1, 1)
            left = jnp.where(lane == 0, before[a, here, :].astype(jnp.float32), left)
            right = jnp.where(lane == columns - 1, after[a, here, :].astype(jnp.float32), right)
            slope_y = above[a, here, :].astype(jnp.float32) - below[a, here, :].astype(jnp.float32)
            slope_z = around[9 : 9 + rows] - around[7 : 7 + rows]
            grad.append([(right - left) * 0.5, slope_y * 0.5, slope_z * 0.5])
        parts, magnitude = strain(grad)
        for p, part in enumerate(parts):
            out[p, here, :] = 4.0 * magnitude * part
        return carry

    lax.fori_loop(0, length // rows, tile, 0)


def coarse_model(hat, below, above, before, after):
    _, length, columns = hat.shape
    vmem = pl.BlockSpec(memory_space=pltpu.VMEM)
    return pl.pallas_call(
        coarse_kernel,
        in_specs=[vmem] * 5,
        out_specs=vmem,
        out_shape=jax.ShapeDtypeStruct((6, length, columns), jnp.float32),
        scratch_shapes=[pltpu.VMEM((3, length + 16, columns), jnp.float32)],
        cost_estimate=pl.CostEstimate(
            flops=100 * length * columns, bytes_accessed=42 * length * columns, transcendentals=0
        ),
    )(hat, below, above, before, after)


def lilly_kernel(n, weight, *refs):
    table, blocks = refs[0], refs[1 : 1 + n]
    product, left, right, coarse, start, out = refs[1 + n :]
    width, columns = blocks[0].shape[1:]
    rows = min(256, product.shape[1])

    @pl.when(pl.program_id(0) == 0)
    def _():
        out[...] = start[...]

    for top in range(0, product.shape[1], rows):
        here = slice(top, top + rows)
        total = None
        for s in range(n):
            term = jnp.dot(
                table[here, s * width : (s + 1) * width],
                blocks[s][0],
                preferred_element_type=jnp.float32,
            )
            total = term if total is None else total + term
        fine = total.astype(jnp.bfloat16).astype(jnp.float32)
        model = fine - coarse[0, here, :]
        leonard = product[0, here, :].astype(jnp.float32) - left[0, here, :].astype(
            jnp.float32
        ) * right[0, here, :].astype(jnp.float32)
        for i, value in enumerate((leonard * model, model * model)):
            out[i] += weight * jnp.sum(value.reshape(rows // 8, 8, columns), axis=0)


def lilly(table, blocks, products, hat, coarse, first, start):
    n, (fields, width, columns) = len(blocks), blocks[0].shape
    length = table.shape[0]
    a0, b0 = index_pairs[first]
    a1, b1 = index_pairs[first + 1] if fields > 1 else (a0, b0)

    def plane(offset, step=1):
        return pl.BlockSpec((1, length, columns), lambda f: (offset + f * step, 0, 0))

    for f in range(fields):
        assert index_pairs[first + f] == (a0 + f * (a1 - a0), b0 + f * (b1 - b0))
        assert pair_weights[first + f] == pair_weights[first]
    sums = pl.BlockSpec(start.shape, lambda f: (0, 0, 0))
    return pl.pallas_call(
        functools.partial(lilly_kernel, n, pair_weights[first]),
        grid=(fields,),
        in_specs=[pl.BlockSpec(table.shape, lambda f: (0, 0), pipeline_mode=pl.Buffered(1))]
        + [pl.BlockSpec((1, width, columns), lambda f: (f, 0, 0))] * n
        + [plane(first), plane(a0, a1 - a0), plane(b0, b1 - b0), plane(first), sums],
        out_specs=sums,
        out_shape=jax.ShapeDtypeStruct(start.shape, jnp.float32),
        cost_estimate=pl.CostEstimate(
            flops=2 * fields * length * length * columns,
            bytes_accessed=12 * fields * length * columns + 2 * length * length,
            transcendentals=0,
        ),
    )(table, *blocks, products, hat, hat, coarse, start)


def coefficient_kernel(n, cells, part, out, held, send_sem, recv_sem):
    me = lax.axis_index("pz")
    barrier = pltpu.get_barrier_semaphore()
    others = [lax.rem(me + s, n) for s in range(1, n)]
    for other in others:
        pl.semaphore_signal(
            barrier, inc=1, device_id={"pz": other}, device_id_type=pl.DeviceIdType.MESH
        )
    pl.semaphore_wait(barrier, n - 1)
    copies = [
        pltpu.make_async_remote_copy(
            src_ref=part,
            dst_ref=held.at[s],
            send_sem=send_sem.at[s],
            recv_sem=recv_sem.at[s],
            device_id={"pz": other},
            device_id_type=pl.DeviceIdType.MESH,
        )
        for s, other in enumerate(others)
    ]
    for copy in copies:
        copy.start()
    total = part[...]
    for s, copy in enumerate(copies):
        copy.wait()
        total = total + held[s]
    mean = jnp.sum(jnp.sum(total, axis=2, keepdims=True), axis=1, keepdims=True) / cells
    value = mean[0] / (2.0 * (mean[1] + epsilon))
    out[...] = jnp.broadcast_to(value, out.shape)


def coefficient_of(part, cells, columns):
    n = lax.axis_size("pz")
    return pl.pallas_call(
        functools.partial(coefficient_kernel, n, cells),
        in_specs=[pl.BlockSpec(memory_space=pltpu.VMEM)],
        out_specs=pl.BlockSpec(memory_space=pltpu.VMEM),
        out_shape=jax.ShapeDtypeStruct((8, columns), jnp.float32),
        scratch_shapes=[
            pltpu.VMEM((n - 1,) + part.shape, jnp.float32),
            pltpu.SemaphoreType.DMA((n - 1,)),
            pltpu.SemaphoreType.DMA((n - 1,)),
        ],
        compiler_params=pltpu.CompilerParams(collective_id=0, has_side_effects=True),
    )(part)


def body(velocity):
    n, me = lax.axis_size("pz"), lax.axis_index("pz")
    v = velocity[:, 0]
    depth, nx = v.shape[1:]
    nz, width = depth * n, nx // n
    table_x = filter_table(nx)
    table_z = table_x if nz == nx else filter_table(nz)
    to_x = [
        lax.dynamic_slice_in_dim(table_x, lax.rem(me + s, n) * width, width, 1) for s in range(n)
    ]
    from_z = jnp.concatenate(
        [
            lax.dynamic_slice_in_dim(table_z, lax.rem(me - s + n, n) * depth, depth, 1)
            for s in range(n)
        ],
        axis=1,
    )
    order = list(range(n - 1, 0, -1))
    order.sort(key=lambda s: -min(s, n - s))

    def exchange(pieces):
        fields = jnp.stack([p.astype(jnp.bfloat16) for p in pieces])
        blocks = [None] * n
        for s in order + [0]:
            along = jnp.einsum(
                "fzx,xv->fzv", fields, to_x[s], preferred_element_type=jnp.float32
            ).astype(jnp.bfloat16)
            if s:
                along = lax.ppermute(along, "pz", [(i, (i + s) % n) for i in range(n)])
            blocks[s] = along
        return blocks

    blocks_v = exchange([v[a] for a in range(3)])
    below, above = neighbours(v, v, "py", False)
    before, after = neighbours(v[:, :1], v[:, -1:], "pz", True)
    blocks_p = exchange([v[a] * v[b] for a, b in index_pairs])

    padded = jnp.concatenate([before, v, after], axis=1)
    slope_x = (jnp.roll(v, -1, 2) - jnp.roll(v, 1, 2)) * 0.5
    slope_y = (above - below) * 0.5
    slope_z = (padded[:, 2:] - padded[:, :-2]) * 0.5
    grad = [[slope_x[a], slope_y[a], slope_z[a]] for a in range(3)]
    parts, magnitude = strain([[g[b] for b in range(3)] for g in grad])
    groups = ((0, 3), (3, 5), (5, 6))
    blocks_s = [
        exchange([magnitude * part for part in parts[first:last]]) for first, last in groups
    ]
    from_z, *local = lax.optimization_barrier((from_z, *[blocks[0] for blocks in blocks_s]))
    for blocks, own in zip(blocks_s, local):
        blocks[0] = own

    hat = filter_z(from_z, blocks_v)
    below, above = neighbours(hat, hat, "py", False)
    before, after = neighbours(hat[:, :, :1], hat[:, :, -1:], "pz", True)
    coarse = coarse_model(hat, below, above, before, after)
    products = filter_z(from_z, blocks_p)
    sums = jnp.zeros((2, 8, width), jnp.float32)
    for (first, _), blocks in zip(groups, blocks_s):
        sums = lilly(from_z, blocks, products, hat, coarse, first, sums)
    coefficient = coefficient_of(sums, nx * nz, nx)
    nu_t = magnitude.reshape(depth // 8, 8, nx) * coefficient
    return nu_t.reshape(1, depth, nx), hat[:, None]


def solution(mesh):
    in_specs = (P(None, "py", "pz", None),)
    out_specs = (P("py", "pz", None), P(None, "py", None, "pz"))
    return jax.shard_map(body, mesh=mesh, in_specs=in_specs, out_specs=out_specs, check_vma=False)
```
